32 devices in a mesh: seq: 32 (over z, y, x, core), head: 1.
Axes of the slice: x: 2, y: 2, z: 4, core: 2. Of those that a mesh axis runs over, the one named last changes fastest.
Arguments:
- queries: bfloat16 [8192, 4096], P('seq', 'head'), may hold values from -8 to 8
- keys: bfloat16 [8192, 1024], P('seq', 'head'), may hold values from -8 to 8
- values: bfloat16 [8192, 1024], P('seq', 'head'), may hold values from -8 to 8
- gate_logit: float32 [32], P('head'), may hold values from -3 to 3
- out_weight: bfloat16 [4096, 4096], P('head'), may hold values from -0.09375 to 0.09375
Outputs:
- layer_out: bfloat16 [8192, 4096], P('seq', 'head')
The draws below stay inside these ranges and needn't reach their ends.
All inputs are finite; a program needn't handle non-finite values.
Results may differ from the reference program's by a relative error of at most 0.0095.
Values may be sent and summed in bfloat16 or wider, within the bound.
A program may use at most 320 MiB of HBM per device.

```python
import math
import jax
import jax.numpy as jnp
from jax import lax

D = 4096
Q_HEADS = 32
KV_HEADS = 8
HDIM = 128
WINDOW = 4096
SEG = 1024
TOK_DEV = 256
TOKENS = 8192


def draw_queries(key, part):
    base_key = jax.random.fold_in(key, 11)
    base_draw = jnp.clip(0.6 * jax.random.normal(base_key, (TOKENS, Q_HEADS, HDIM), jnp.float32), -8.0, 8.0)
    return base_draw.reshape(TOKENS, Q_HEADS * HDIM).astype(jnp.bfloat16)


def draw_keys(key, part):
    scale_key = jax.random.fold_in(key, 21)
    token_key = jax.random.fold_in(key, 22)
    base_key = jax.random.fold_in(key, 23)
    block_scale = jnp.exp(jax.random.uniform(scale_key, (TOKENS // TOK_DEV, KV_HEADS), jnp.float32, math.log(0.3), math.log(3.0)))
    block_scale = jnp.repeat(block_scale, TOK_DEV, axis=0)
    token_scale = jnp.exp(jax.random.uniform(token_key, (TOKENS, KV_HEADS), jnp.float32, math.log(0.6), math.log(1.6)))
    row_scale = (block_scale * token_scale)[:, :, None]
    base_draw = jax.random.normal(base_key, (TOKENS, KV_HEADS, HDIM), jnp.float32)
    base_draw = jnp.clip(base_draw * row_scale, -8.0, 8.0)
    return base_draw.reshape(TOKENS, KV_HEADS * HDIM).astype(jnp.bfloat16)


def draw_values(key, part):
    offset_key = jax.random.fold_in(key, 31)
    base_key = jax.random.fold_in(key, 32)
    offsets = jax.random.uniform(offset_key, (TOKENS // TOK_DEV, KV_HEADS * HDIM), jnp.float32, -1.0, 1.0)
    offsets = jnp.repeat(offsets, TOK_DEV, axis=0)
    base_draw = jax.random.normal(base_key, (TOKENS, KV_HEADS * HDIM), jnp.float32)
    return jnp.clip(base_draw + offsets, -8.0, 8.0).astype(jnp.bfloat16)


def centred(own_key, extent, width, limit, held_as=jnp.bfloat16):
    return jnp.clip(width * jax.random.normal(own_key, extent, jnp.float32), -limit, limit).astype(held_as)


def setup_inputs(seed: int = 0) -> dict:
    seeds = jax.random.split(jax.random.key(seed), 6)
    return {
        "queries": draw_queries(jax.random.fold_in(seeds[5], 71), 0),
        "keys": draw_keys(jax.random.fold_in(seeds[5], 71), 0),
        "values": draw_values(jax.random.fold_in(seeds[5], 71), 0),
        "gate_logit": jnp.clip(jax.random.uniform(seeds[3], (Q_HEADS,), jnp.float32, -3.0, 3.0), -3.0, 3.0),
        "out_weight": centred(seeds[4], (Q_HEADS * HDIM, D), (Q_HEADS * HDIM) ** -0.5, 0.09375),
    }


def feature(source):
    return jax.nn.elu(source.astype(jnp.float32)) + 1.0

def reference(queries, keys, values, gate_logit, out_weight):
    group_size = Q_HEADS // KV_HEADS
    score_scale = 1.0 / math.sqrt(HDIM)
    query_four = queries.reshape(TOKENS, KV_HEADS, group_size, HDIM)
    key_three = keys.reshape(TOKENS, KV_HEADS, HDIM)
    value_three = values.reshape(TOKENS, KV_HEADS, HDIM)
    padding = jnp.zeros((WINDOW, KV_HEADS, HDIM), jnp.bfloat16)
    key_padded = jnp.concatenate([padding, key_three], 0)
    value_padded = jnp.concatenate([padding, value_three], 0)

    def attend_block(block):
        first = (block * TOK_DEV).astype(jnp.int32)
        query_rows = lax.dynamic_slice_in_dim(query_four, first, TOK_DEV, 0).astype(jnp.float32)
        key_rows = lax.dynamic_slice_in_dim(key_padded, first, WINDOW + TOK_DEV, 0).astype(jnp.float32)
        value_rows = lax.dynamic_slice_in_dim(value_padded, first, WINDOW + TOK_DEV, 0).astype(jnp.float32)
        query_pos = first + jnp.arange(TOK_DEV, dtype=jnp.int32)
        key_pos = first - WINDOW + jnp.arange(WINDOW + TOK_DEV, dtype=jnp.int32)
        distance = query_pos[:, None] - key_pos[None, :]
        allowed = (distance >= 0) & (distance < WINDOW) & (key_pos[None, :] >= 0)
        scores = jnp.einsum('tgrd,sgd->tgrs', query_rows, key_rows) * score_scale
        scores = jnp.where(allowed[:, None, None, :], scores, jnp.float32(-1e+30))
        peak = lax.optimization_barrier(jnp.max(scores, axis=-1, keepdims=True))
        weights = jnp.exp(scores - peak)
        sum_total = lax.optimization_barrier(jnp.sum(weights, axis=-1))
        low = weights.astype(jnp.bfloat16).astype(jnp.float32)
        weighted = jnp.einsum('tgrs,sgd->tgrd', low, value_rows)
        return weighted / sum_total[..., None]
    local_out = lax.map(attend_block, jnp.arange(TOKENS // TOK_DEV, dtype=jnp.int32))
    local_out = local_out.reshape(TOKENS, KV_HEADS, group_size, HDIM)
    seg_count = TOKENS // SEG
    key_feature = feature(key_three).astype(jnp.bfloat16).astype(jnp.float32).reshape(seg_count, SEG, KV_HEADS, HDIM)
    value_seg = value_three.astype(jnp.float32).reshape(seg_count, SEG, KV_HEADS, HDIM)
    delta_memory = jnp.einsum('nsgd,nsge->ngde', key_feature, value_seg, precision=lax.Precision.HIGHEST)
    delta_norm = lax.optimization_barrier(jnp.sum(key_feature, axis=1))
    memory = jnp.concatenate([jnp.zeros((1, KV_HEADS, HDIM, HDIM), jnp.float32), jnp.cumsum(delta_memory, 0)[:-1]], 0)
    key_total = jnp.concatenate([jnp.zeros((1, KV_HEADS, HDIM), jnp.float32), jnp.cumsum(delta_norm, 0)[:-1]], 0)
    query_feature = feature(query_four).astype(jnp.bfloat16).astype(jnp.float32).reshape(seg_count, SEG, KV_HEADS, group_size, HDIM)
    recalled = jnp.einsum('nsgrd,ngde->nsgre', query_feature, memory, precision=lax.Precision.HIGHEST)
    denominator = 1.0 + jnp.einsum('nsgrd,ngd->nsgr', query_feature, key_total, precision=lax.Precision.HIGHEST)
    retrieved = (recalled / denominator[..., None]).reshape(TOKENS, KV_HEADS, group_size, HDIM)
    gate_share = jax.nn.sigmoid(gate_logit.astype(jnp.float32)).reshape(KV_HEADS, group_size)[None, :, :, None]
    mixed = (gate_share * retrieved + (1.0 - gate_share) * local_out).astype(jnp.bfloat16)
    mixed = mixed.reshape(TOKENS, Q_HEADS * HDIM)
    return jnp.dot(mixed, out_weight, preferred_element_type=jnp.float32).astype(jnp.bfloat16)
```

```python
import functools
import math

import jax
import jax.numpy as jnp
from jax import lax
from jax.experimental import pallas as pl
from jax.experimental.pallas import tpu as pltpu
from jax.sharding import PartitionSpec as P

HDIM = 128
WINDOW = 4096
SEG = 1024
LOG2E = 1.4426950408889634
EXP_SCALE = LOG2E / math.sqrt(HDIM)


def feature(source):
    wide = source.astype(jnp.float32)
    low = jnp.exp(jnp.minimum(wide, 0.0))
    return jnp.where(wide > 0.0, wide + 1.0, low)


def kernel(
    size, group_size, gate_ref, q_ref, k_hbm, v_hbm, out_ref,
    kbuf, vbuf, m_ref, acc_ref, wsend, wrecv, dsum, dpre,
    local_sem, send_sem, recv_sem, zsend, zrecv, dsend, drecv,
):
    rows = q_ref.shape[0]
    width = kbuf.shape[2]
    groups = width // HDIM
    me = lax.axis_index("seq")
    plane = me // 8
    p = me % 8
    core = p % 2
    xbit = (p // 2) % 2
    ybit = p // 4
    base = me - p
    by_core = 1 - 2 * core
    by_x = 2 - 4 * xbit
    by_y = 4 - 8 * ybit
    dev_core, dev_x, dev_y = me + by_core, me + by_x, me + by_y
    slots = (p, p + by_x, p + by_y, p + by_x + by_y)
    bufs = (kbuf, vbuf)
    X_FIRST = ((True, True), (True, False), (True, False))

    has_up = me + 8 < size
    has_down = plane >= 1

    def rows_of(slot):
        return pl.ds(pl.multiple_of(slot * rows, rows), rows)

    def remote(src, dst, ssem, rsem, dev):
        return pltpu.make_async_remote_copy(
            src_ref=src, dst_ref=dst, send_sem=ssem, recv_sem=rsem,
            device_id={"seq": dev}, device_id_type=pl.DeviceIdType.MESH,
        )

    def hop(g, kv, slot, dev, idx):
        ref = bufs[kv].at[g, rows_of(slot), :]
        return remote(ref, ref, send_sem.at[g, kv, idx], recv_sem.at[g, kv, idx], dev)

    def up(g, kv):
        src = bufs[kv].at[g, rows_of(p), :]
        dst = bufs[kv].at[g + 1, rows_of(p), :]
        return remote(src, dst, zsend.at[g, kv], zrecv.at[g, kv], me + 8)

    def first_step(g, kv):
        return hop(g, kv, slots[0], dev_x if X_FIRST[g][kv] else dev_y, 0)

    def second_step(g, kv, which):
        if X_FIRST[g][kv]:
            return hop(g, kv, slots[(0, 1)[which]], dev_y, 1 + which)
        return hop(g, kv, slots[(0, 2)[which]], dev_x, 1 + which)

    def core_step(g, kv, which):
        return hop(g, kv, slots[which], dev_core, 3 + which)

    def sends_y(g):
        return (ybit == 0, ybit < 2, ybit == 1)[g]

    def far(g):
        return (ybit == 1, ybit < 2, ybit == 0)[g]

    def has(g):
        return plane >= g

    def conds(g, kv, idx):
        y_send, y_recv = has(g) & sends_y(g), has(g) & far(g)
        both = (has(g), has(g))
        if idx == 0:
            return both if X_FIRST[g][kv] else (y_send, y_recv)
        if idx in (1, 2):
            if X_FIRST[g][kv]:
                return (y_send, y_recv)
            return both if idx == 1 else (y_recv, y_recv)
        return both if idx in (3, 4) else (y_recv, y_recv)

    def copy_of(g, kv, idx):
        if idx == 0:
            return first_step(g, kv)
        if idx in (1, 2):
            return second_step(g, kv, idx - 1)
        return core_step(g, kv, idx - 3)

    def start(g, kv, idx):
        @pl.when(conds(g, kv, idx)[0])
        def _():
            copy_of(g, kv, idx).start()

    def arrive(g, kv, idx):
        @pl.when(conds(g, kv, idx)[1])
        def _():
            copy_of(g, kv, idx).wait_recv()

    def exchange(i, value):
        dev = (dev_core, dev_x, dev_y)[i]
        wsend[i] = value.astype(jnp.bfloat16)
        remote(wsend.at[i], wrecv.at[i], dsend.at[i], drecv.at[i], dev).start()

    def exchanged(i):
        dev = (dev_core, dev_x, dev_y)[i]
        remote(wsend.at[i], wrecv.at[i], dsend.at[i], drecv.at[i], dev).wait_recv()
        return wrecv[i].astype(jnp.float32)

    def chain():
        return remote(wsend.at[3], wrecv.at[3], dsend.at[3], drecv.at[3], me + 8)

    def attend(g, chunk, masked=False):
        first_row = pl.multiple_of(chunk * (2 * rows), 2 * rows)
        ones = jnp.ones((2 * rows, HDIM), jnp.bfloat16)
        if masked:
            qpos = lax.broadcasted_iota(jnp.int32, (rows, 2 * rows), 0) + p * rows
            kpos = lax.broadcasted_iota(jnp.int32, (rows, 2 * rows), 1) + first_row
            allowed = (qpos >= kpos) if g == 0 else (kpos > qpos)

        def head(h, carry):
            cols = pl.ds(pl.multiple_of(h * HDIM, HDIM), HDIM)
            k = kbuf[g, pl.ds(first_row, 2 * rows), cols]
            v = vbuf[g, pl.ds(first_row, 2 * rows), cols]
            v_wide = jnp.concatenate([v, ones], axis=1)
            for r in range(group_size):
                n = h * group_size + r
                q = q_ref[:, pl.ds(pl.multiple_of(n * HDIM, HDIM), HDIM)]
                s = lax.dot_general(
                    q, k, (((1,), (1,)), ((), ())), preferred_element_type=jnp.float32
                )
                if masked:
                    s = jnp.where(allowed, s, jnp.float32(-1e30))
                old = m_ref[n]
                new = jnp.maximum(old, jnp.max(s, axis=1, keepdims=True))
                m_ref[n] = new
                alpha = jnp.exp2((old - new) * EXP_SCALE)
                shift = jnp.concatenate([new] * (2 * rows // HDIM), axis=1)
                w = jnp.exp2((s - shift) * EXP_SCALE).astype(jnp.bfloat16)
                pv = jnp.dot(w, v_wide, preferred_element_type=jnp.float32)
                acc_ref[n] = acc_ref[n] * jnp.concatenate([alpha, alpha], axis=1) + pv
            return carry

        lax.fori_loop(0, groups, head, 0)

    own_chunk = p // 2
    near_chunk = own_chunk + 1 - 2 * xbit
    far_base = 2 - 2 * ybit
    KV = (0, 1)

    local = [
        pltpu.make_async_copy(hbm, buf.at[0, rows_of(p), :], local_sem.at[i])
        for i, (hbm, buf) in enumerate(((k_hbm, kbuf), (v_hbm, vbuf)))
    ]
    for c in local:
        c.start()
    barrier = pltpu.get_barrier_semaphore()
    for dev in (dev_core, dev_x, dev_y):
        pl.semaphore_signal(
            barrier, inc=1, device_id={"seq": dev}, device_id_type=pl.DeviceIdType.MESH
        )

    @pl.when(has_up)
    def _():
        pl.semaphore_signal(
            barrier, inc=1, device_id={"seq": me + 8}, device_id_type=pl.DeviceIdType.MESH
        )

    @pl.when(has_down)
    def _():
        pl.semaphore_signal(
            barrier, inc=1, device_id={"seq": me - 8}, device_id_type=pl.DeviceIdType.MESH
        )

    steps = max(size // 8 - 1, 1)
    neighbours_up = 1 - plane // steps if size > 8 else 0
    neighbours_down = (plane + steps - 1) // steps if size > 8 else 0
    pl.semaphore_wait(barrier, 3 + neighbours_up + jnp.minimum(neighbours_down, 1))

    for c in local:
        c.wait()

    for kv in KV:
        start(0, kv, 3)
    for kv in KV:
        @pl.when(has_up)
        def _(kv=kv):
            up(0, kv).start()

        start(0, kv, 0)
    m_ref[...] = jnp.full(m_ref.shape, -1e30, jnp.float32)
    acc_ref[...] = jnp.zeros(acc_ref.shape, jnp.float32)
    for h in range(groups):
        cols = slice(h * HDIM, (h + 1) * HDIM)
        kf = feature(kbuf[0, rows_of(p), cols]).astype(jnp.bfloat16)
        v = vbuf[0, rows_of(p), cols]
        dsum[0:HDIM, cols] = lax.dot_general(
            kf, v, (((0,), (0,)), ((), ())), preferred_element_type=jnp.float32
        )
        norm = jnp.sum(kf.astype(jnp.float32), axis=0, keepdims=True)
        dsum[HDIM:, cols] = jnp.broadcast_to(norm, (dsum.shape[0] - HDIM, HDIM))
    exchange(0, dsum[...])
    for kv in KV:
        arrive(0, kv, 3)
    attend(0, own_chunk, masked=True)
    dsum[...] += exchanged(0)
    exchange(1, dsum[...])

    for kv in KV:
        arrive(0, kv, 0)
        start(0, kv, 4)

    @pl.when(has(1))
    def _():
        for kv in KV:
            up(0, kv).wait_recv()

    for kv in KV:
        start(1, kv, 3)
        start(1, kv, 0)

        @pl.when(has(1) & has_up)
        def _(kv=kv):
            up(1, kv).start()

    for kv in KV:
        arrive(0, kv, 4)

    @pl.when(xbit == 1)
    def _():
        attend(0, near_chunk)

    for kv in KV:
        arrive(1, kv, 3)

    @pl.when(has(1))
    def _():
        attend(1, own_chunk)

    dsum[...] += exchanged(1)
    exchange(2, dsum[...])

    for kv in KV:
        arrive(1, kv, 0)
        start(1, kv, 1)
        start(1, kv, 2)
        start(1, kv, 4 if X_FIRST[1][kv] else 5)
    for kv in KV:
        start(0, kv, 1)
        start(0, kv, 2)

    @pl.when(has(2))
    def _():
        for kv in KV:
            up(1, kv).wait_recv()

    for kv in KV:
        start(2, kv, 3)
        start(2, kv, 0)
    other = exchanged(2)
    dpre[...] = other * ybit.astype(jnp.float32)
    dsum[...] += other

    @pl.when(has_up & (plane == 0))
    def _():
        wsend[3] = dsum[...].astype(jnp.bfloat16)
        chain().start()

    for kv in KV:
        arrive(2, kv, 3)

    @pl.when(has(2))
    def _():
        attend(2, own_chunk, masked=True)

    @pl.when(has_down)
    def _():
        chain().wait_recv()
        before = wrecv[3].astype(jnp.float32)
        dpre[...] += before

        @pl.when(has_up)
        def _():
            wsend[3] = (before + dsum[...]).astype(jnp.bfloat16)
            chain().start()

    for kv in KV:
        arrive(1, kv, 1)
        arrive(1, kv, 2)
        start(1, kv, 5 if X_FIRST[1][kv] else 4)
        start(1, kv, 6)
    for kv in KV:
        arrive(2, kv, 0)
        start(2, kv, 1)
        start(2, kv, 2)
        start(2, kv, 4 if X_FIRST[2][kv] else 5)
    for kv in KV:
        arrive(1, kv, 4)
        arrive(1, kv, 5)
        arrive(1, kv, 6)

    @pl.when(has(1))
    def _():
        def one(i, c):
            attend(1, (own_chunk + 1 + i) % 4)
            return c

        lax.fori_loop(0, 3, one, 0)

    for kv in KV:
        arrive(2, kv, 1)
        arrive(2, kv, 2)
        start(2, kv, 5 if X_FIRST[2][kv] else 4)
        start(2, kv, 6)
    for kv in KV:
        arrive(2, kv, 4)
        arrive(2, kv, 5)
        arrive(2, kv, 6)

    @pl.when(has(2) & (xbit == 0))
    def _():
        attend(2, near_chunk)

    for kv in KV:
        arrive(0, kv, 1)
        arrive(0, kv, 2)
        start(0, kv, 5)
        start(0, kv, 6)
    for kv in KV:
        arrive(0, kv, 5)
        arrive(0, kv, 6)

    @pl.when(far(0))
    def _():
        lax.fori_loop(0, 2, lambda i, c: (attend(0, far_base + i), c)[1], 0)

    @pl.when(has(2) & far(2))
    def _():
        lax.fori_loop(0, 2, lambda i, c: (attend(2, far_base + i), c)[1], 0)

    def finish(h, carry):
        cols = pl.ds(pl.multiple_of(h * HDIM, HDIM), HDIM)
        mem = dpre[0:HDIM, cols]
        high = mem.astype(jnp.bfloat16)
        low = (mem - high.astype(jnp.float32)).astype(jnp.bfloat16)
        norm = dpre[HDIM:HDIM + 1, cols]
        for r in range(group_size):
            n = h * group_size + r
            qcols = pl.ds(pl.multiple_of(n * HDIM, HDIM), HDIM)
            qf = feature(q_ref[:, qcols]).astype(jnp.bfloat16)
            recalled = jnp.dot(qf, high, preferred_element_type=jnp.float32) + jnp.dot(
                qf, low, preferred_element_type=jnp.float32
            )
            denominator = 1.0 + jnp.sum(qf.astype(jnp.float32) * norm, axis=1, keepdims=True)
            local_out = acc_ref[n, :, 0:HDIM] / acc_ref[n, :, HDIM:]
            share = gate_ref[n]
            mixed = share * (recalled / denominator) + (1.0 - share) * local_out
            out_ref[:, qcols] = mixed.astype(jnp.bfloat16)
        return carry

    lax.fori_loop(0, groups, finish, 0)

    for i, dev in enumerate((dev_core, dev_x, dev_y)):
        remote(wsend.at[i], wrecv.at[i], dsend.at[i], drecv.at[i], dev).wait_send()

    @pl.when(has_up)
    def _():
        chain().wait_send()
        for kv in KV:
            up(0, kv).wait_send()

    @pl.when(has_up & has(1))
    def _():
        for kv in KV:
            up(1, kv).wait_send()

    for g in range(3):
        for kv in KV:
            for idx in range(7):
                @pl.when(conds(g, kv, idx)[0])
                def _(g=g, kv=kv, idx=idx):
                    copy_of(g, kv, idx).wait_send()


def per_device(size, queries, keys, values, gate_logit, out_weight):
    rows = queries.shape[0]
    heads = gate_logit.shape[0]
    width = keys.shape[1]
    group_size = heads // (width // HDIM)
    assert WINDOW == 16 * rows and SEG == 4 * rows and size % 8 == 0
    vmem, anywhere = pl.BlockSpec(memory_space=pltpu.VMEM), pl.BlockSpec(memory_space=pl.ANY)
    mixed = pl.pallas_call(
        functools.partial(kernel, size, group_size),
        out_shape=jax.ShapeDtypeStruct(queries.shape, jnp.bfloat16),
        in_specs=[pl.BlockSpec(memory_space=pltpu.SMEM), vmem, anywhere, anywhere],
        out_specs=vmem,
        scratch_shapes=[
            pltpu.VMEM((3, 8 * rows, width), jnp.bfloat16),
            pltpu.VMEM((3, 8 * rows, width), jnp.bfloat16),
            pltpu.VMEM((heads, rows, HDIM), jnp.float32),
            pltpu.VMEM((heads, rows, 2 * HDIM), jnp.float32),
            pltpu.VMEM((4, HDIM + 16, width), jnp.bfloat16),
            pltpu.VMEM((4, HDIM + 16, width), jnp.bfloat16),
            pltpu.VMEM((HDIM + 16, width), jnp.float32),
            pltpu.VMEM((HDIM + 16, width), jnp.float32),
            pltpu.SemaphoreType.DMA((2,)),
            pltpu.SemaphoreType.DMA((3, 2, 7)),
            pltpu.SemaphoreType.DMA((3, 2, 7)),
            pltpu.SemaphoreType.DMA((2, 2)),
            pltpu.SemaphoreType.DMA((2, 2)),
            pltpu.SemaphoreType.DMA((4,)),
            pltpu.SemaphoreType.DMA((4,)),
        ],
        compiler_params=pltpu.CompilerParams(
            collective_id=0, has_side_effects=True, vmem_limit_bytes=60 * 1024 * 1024
        ),
    )(jax.nn.sigmoid(gate_logit), queries, keys, values)
    partial_value = jnp.dot(mixed, out_weight, preferred_element_type=jnp.float32)
    return lax.psum_scatter(
        partial_value.astype(jnp.bfloat16), "head", scatter_dimension=1, tiled=True
    )


def solution(mesh):
    in_specs = (P("seq", "head"), P("seq", "head"), P("seq", "head"), P("head"), P("head", None))
    out_specs = P("seq", "head")
    return jax.shard_map(
        functools.partial(per_device, mesh.shape["seq"]),
        mesh=mesh, in_specs=in_specs, out_specs=out_specs, check_vma=False,
    )
```
